128 devices in a mesh: seq: 32 (over y, z, core), batch: 4 (over x).
Axes of the slice: x: 4, y: 4, z: 4, core: 2. Of those that a mesh axis runs over, the one named last changes fastest.
Arguments:
- queries: bfloat16 [4, 4096, 4096], P('batch', 'seq'), may hold values from -130 to 130
- keys: bfloat16 [4, 4096, 1024], P('batch', 'seq'), may hold values from -4 to 4
- values: bfloat16 [4, 4096, 1024], P('batch', 'seq'), may hold values from -4 to 4
- lengths: int32 [4], P('batch'), may hold values from 2048 to 4096
- block_pos: int32 [4, 32], P('batch'), may hold values from 0 to 31, each once within a row
- w_in: bfloat16 [6144, 1024], replicated, may hold values from -0.078125 to 0.078125
- b_in: float32 [1024], replicated, may hold values from -3 to 3
- output_weight: bfloat16 [1024, 8], replicated, may hold values from -0.1875 to 0.1875
- output_bias: float32 [8], replicated, may hold values from 1 to 2
Outputs:
- grad_w_in: float32 [6144, 1024], P(('seq', 'batch'))
- grad_b_in: float32 [1024], replicated
- output_weight_gradient: float32 [1024, 8], replicated
- output_bias_gradient: float32 [8], replicated
The draws below stay inside these ranges and needn't reach their ends.
Inputs may be any that keep to these rules, and one draw needn't show every extreme that they name: Each row of block_pos names every block 0 to 31 once.
All inputs are finite; a program needn't handle non-finite values.
Results may differ from the reference program's by a relative error of at most 0.0017.
The reference program's roundings to bfloat16 on the way (of `features`, `act`, `resid` and `delta`) count: a program that leaves them out, or rounds other values in their place, can miss the bound.
Values may be sent and summed in bfloat16 or wider, within the bound.
No kernel may reach another device: no remote copies, remote signals or barrier semaphores. Data moves between devices by JAX's collectives and lax.ppermute only.
A program may use at most 128 MiB of HBM per device.

```python
import math
import jax
import jax.numpy as jnp
from jax import lax

QUERY_HEADS = 32
KEY_VALUE_HEADS = 8
HEAD_DIMENSION = 128
HIDDEN_UNITS = 1024
SEQ_DEV = 128
KD = 1024
FEAT = 6144
TOKEN_COUNT = 4096
SEQUENCE_COUNT = 4
N_SEQ = 32


def group_keys(key):
    base_offset = jax.random.fold_in(key, 7301)
    return jnp.clip(jax.random.normal(base_offset, (SEQUENCE_COUNT, TOKEN_COUNT, KEY_VALUE_HEADS * HEAD_DIMENSION), jnp.float32), -4.0, 4.0)


def draw_keys(key, part):
    base_offset = group_keys(key)
    return base_offset.astype(jnp.bfloat16)


def draw_queries(key, part):
    fresh = jax.random.fold_in(key, 1709)
    base_offset = jnp.clip(jax.random.normal(fresh, (SEQUENCE_COUNT, TOKEN_COUNT, QUERY_HEADS * HEAD_DIMENSION), jnp.float32), -4.0, 4.0)
    return base_offset.astype(jnp.bfloat16)


def place_ends(entries, stream_key, least, largest):
    index_at = [jax.random.randint(jax.random.fold_in(stream_key, axis), (), 0, length) for axis, length in enumerate(entries.shape)]
    widest = entries.shape.index(max(entries.shape))
    next_to = index_at[:widest] + [(index_at[widest] + 1) % entries.shape[widest]] + index_at[widest + 1:]
    return entries.at[tuple(index_at)].set(least).at[tuple(next_to)].set(largest)


def shard_levels(stream_key, shape, pieces, least, high):
    gain = 1.0
    for dim, blocks in pieces:
        steps = jax.random.uniform(jax.random.fold_in(jax.random.fold_in(stream_key, 6), dim), (blocks,), jnp.float32, least / len(pieces), high / len(pieces))
        gain = gain * jnp.repeat(jnp.exp(steps), shape[dim] // blocks).reshape((-1,) + (1,) * (len(shape) - 1 - dim))
    return gain


def bell_draw(stream_key, dims, scale, most, split=(), kind=jnp.bfloat16):
    array = jax.random.normal(stream_key, dims, jnp.float32) * scale
    if len(split) > 0:
        array = shard_levels(stream_key, dims, split, -0.22, 0.18) * array
    return jnp.clip(array, min=-most, max=most).astype(kind)


def setup_inputs(seed: int = 0) -> dict:
    seeds = jax.random.split(jax.random.key(seed), 10)
    queries = draw_queries(jax.random.fold_in(seeds[9], 71), 0)
    keys = draw_keys(jax.random.fold_in(seeds[9], 71), 0)
    values = bell_draw(seeds[2], (SEQUENCE_COUNT, TOKEN_COUNT, KD), 1.0, 4.0, ((0, 4), (1, 32)))
    lengths = place_ends(jax.random.randint(seeds[3], (SEQUENCE_COUNT,), TOKEN_COUNT // 2, TOKEN_COUNT + 1), jax.random.fold_in(seeds[3], 1), TOKEN_COUNT // 2, TOKEN_COUNT).astype(jnp.int32)
    block_pos = jax.vmap(lambda own: jax.random.permutation(own, N_SEQ))(jax.random.split(seeds[4], SEQUENCE_COUNT)).reshape((SEQUENCE_COUNT, N_SEQ)).astype(jnp.int32)
    w_in = bell_draw(seeds[5], (FEAT, HIDDEN_UNITS), FEAT ** -0.5, 0.078125)
    b_in = bell_draw(seeds[6], (HIDDEN_UNITS,), 0.5, 3.0, (), jnp.float32)
    output_weight = bell_draw(seeds[7], (HIDDEN_UNITS, KEY_VALUE_HEADS), HIDDEN_UNITS ** -0.5, 0.1875)
    output_bias = jnp.clip(jax.random.uniform(seeds[8], (KEY_VALUE_HEADS,), jnp.float32, 1.0, 2.0), 1.0, 2.0)
    return {"queries": queries, "keys": keys, "values": values, "lengths": lengths, "block_pos": block_pos, "w_in": w_in, "b_in": b_in, "output_weight": output_weight, "output_bias": output_bias}


def column_mass(q_rows, k_rows, positions, limit):
    group_index = QUERY_HEADS // KEY_VALUE_HEADS
    scale = 1.0 / math.sqrt(HEAD_DIMENSION)

    def queries_per_group(g, sums):
        g32 = jnp.asarray(g).astype(jnp.int32)
        k_part = lax.dynamic_slice_in_dim(k_rows, g32 * HEAD_DIMENSION, HEAD_DIMENSION, 1).astype(jnp.float32)
        key_live = positions < limit

        def per_block(i, column):
            i32 = jnp.asarray(i).astype(jnp.int32)
            start = i32 * SEQ_DEV
            q_part = lax.dynamic_slice(q_rows, (start, g32 * group_index * HEAD_DIMENSION), (SEQ_DEV, group_index * HEAD_DIMENSION))
            q_part = q_part.astype(jnp.float32).reshape(SEQ_DEV, group_index, HEAD_DIMENSION)
            q_pos = lax.dynamic_slice_in_dim(positions, start, SEQ_DEV)
            allowed = (positions[None, :] <= q_pos[:, None]) & key_live[None, :]
            scores = jnp.einsum('qhd,kd->hqk', q_part, k_part) * scale
            masked = jnp.where(allowed[None], scores, -1e+30)
            top = lax.optimization_barrier(jnp.max(masked, axis=2, keepdims=True))
            weights = jnp.where(allowed[None], jnp.exp(masked - top), 0.0)
            total = lax.optimization_barrier(jnp.sum(weights, axis=2, keepdims=True))
            q_live = (q_pos < limit).astype(jnp.float32)
            share = weights / total * q_live[None, :, None]
            return column + lax.optimization_barrier(jnp.sum(share, axis=(0, 1)))
        column = lax.fori_loop(0, N_SEQ, per_block, jnp.zeros((TOKEN_COUNT,), jnp.float32))
        return lax.dynamic_update_index_in_dim(sums, column, g32, 0)
    return lax.fori_loop(0, KEY_VALUE_HEADS, queries_per_group, jnp.zeros((KEY_VALUE_HEADS, TOKEN_COUNT), jnp.float32))

def reference(queries, keys, values, lengths, block_pos, w_in, b_in, output_weight, output_bias):
    norm = 1.0 / math.sqrt(SEQUENCE_COUNT * TOKEN_COUNT)
    offsets = jnp.arange(SEQ_DEV, dtype=jnp.int32)
    grad_w_in = jnp.zeros((FEAT, HIDDEN_UNITS), jnp.float32)
    grad_b_in = jnp.zeros((HIDDEN_UNITS,), jnp.float32)
    output_weight_gradient = jnp.zeros((HIDDEN_UNITS, KEY_VALUE_HEADS), jnp.float32)
    output_bias_gradient = jnp.zeros((KEY_VALUE_HEADS,), jnp.float32)
    for index in range(SEQUENCE_COUNT):
        q_rows = queries[index]
        k_rows = keys[index]
        v_rows = values[index]
        positions = (block_pos[index][:, None] * SEQ_DEV + offsets[None, :]).reshape(-1).astype(jnp.int32)
        limit = lengths[index]
        live = (positions < limit).astype(jnp.float32)
        mass = column_mass(q_rows, k_rows, positions, limit)
        labels = jnp.log1p(mass).T
        features = jnp.concatenate([q_rows, k_rows, v_rows], axis=1)
        pre = jnp.dot(features, w_in, preferred_element_type=jnp.float32) + b_in
        act = jax.nn.silu(pre).astype(jnp.bfloat16)
        pred = jnp.dot(act, output_weight, preferred_element_type=jnp.float32) + output_bias
        resid = ((pred - labels) * live[:, None] * norm).astype(jnp.bfloat16)
        back = jnp.dot(resid, output_weight.T, preferred_element_type=jnp.float32)
        sig = jax.nn.sigmoid(pre)
        delta = (back * sig * (1.0 + pre * (1.0 - sig))).astype(jnp.bfloat16)
        grad_w_in = grad_w_in + jnp.dot(features.T, delta, preferred_element_type=jnp.float32)
        grad_b_in = grad_b_in + lax.optimization_barrier(jnp.sum(delta.astype(jnp.float32), axis=0))
        output_weight_gradient = output_weight_gradient + jnp.dot(act.T, resid, preferred_element_type=jnp.float32)
        output_bias_gradient = output_bias_gradient + lax.optimization_barrier(jnp.sum(resid.astype(jnp.float32), axis=0))
    return (grad_w_in, grad_b_in, output_weight_gradient, output_bias_gradient)
```

```python
import functools
import math

import jax
import jax.numpy as jnp
from jax import lax
from jax.experimental import pallas as pl
from jax.experimental.pallas import tpu as pltpu
from jax.sharding import PartitionSpec as P

BLOCK = 128
CHUNK = 256


def mass_kernel(order_ref, where_ref, limit_ref, q_ref, k_ref, out_ref, keys, scores, col, high, *, scale):
    blocks = q_ref.shape[0] // BLOCK
    per = CHUNK // BLOCK
    limit = limit_ref[0]
    factor = scale * math.log2(math.e)

    def by_position(p, carry):
        start = pl.multiple_of(where_ref[p] * BLOCK, BLOCK)
        keys[pl.ds(pl.multiple_of(p * BLOCK, BLOCK), BLOCK), :] = k_ref[pl.ds(start, BLOCK), :]
        return carry

    lax.fori_loop(0, blocks, by_position, 0)
    col[...] = jnp.zeros_like(col)
    row = lax.broadcasted_iota(jnp.int32, (CHUNK, CHUNK), 0)
    column = lax.broadcasted_iota(jnp.int32, (CHUNK, CHUNK), 1)

    def folded(tile, op):
        out = tile[:, :BLOCK]
        for i in range(1, per):
            out = op(out, tile[:, i * BLOCK : (i + 1) * BLOCK])
        return out

    def row_block(r, carry):
        parts = [
            q_ref[pl.ds(pl.multiple_of(where_ref[r * per + i] * BLOCK, BLOCK), BLOCK), :] for i in range(per)
        ]
        q_rows = jnp.concatenate(parts, axis=0)

        def product(c):
            k_rows = keys[pl.ds(pl.multiple_of(c * CHUNK, CHUNK), CHUNK), :]
            return lax.dot_general(
                q_rows, k_rows, (((1,), (1,)), ((), ())), preferred_element_type=jnp.float32
            )

        own = jnp.where((column <= row) & (column + r * CHUNK < limit), product(r), -1e30)
        scores[r] = own
        high[...] = folded(own, jnp.maximum)

        def score_step(c, carry):
            tile = product(c)
            scores[c] = tile
            high[...] = jnp.maximum(high[...], folded(tile, jnp.maximum))
            return carry

        lax.fori_loop(0, r, score_step, 0)
        top = jnp.max(high[...], axis=1, keepdims=True)
        high[...] = jnp.zeros_like(high)

        def exp_step(c, carry):
            tile = jnp.exp2((scores[c] - top) * factor)
            scores[c] = tile
            high[...] += folded(tile, jnp.add)
            return carry

        lax.fori_loop(0, r + 1, exp_step, 0)
        total = jnp.sum(high[...], axis=1, keepdims=True)
        live = lax.broadcasted_iota(jnp.int32, (CHUNK, 1), 0) + r * CHUNK < limit
        weight = jnp.where(live, 1.0 / total, 0.0)

        def column_step(c, carry):
            tile = scores[c] * weight
            part = jnp.sum(tile.reshape(CHUNK // 8, 8, CHUNK), axis=0)
            for i in range(per):
                col[c * per + i] += part[:, i * BLOCK : (i + 1) * BLOCK]
            return carry

        lax.fori_loop(0, r + 1, column_step, 0)
        return carry

    lax.fori_loop(0, (limit + CHUNK - 1) // CHUNK, row_block, 0)

    def store(i, carry):
        out_ref[i] = col[order_ref[i]]
        return carry

    lax.fori_loop(0, blocks, store, 0)


def head_mass(order, where, limit, q_rows, k_rows, scale):
    tokens, size = q_rows.shape
    blocks = tokens // BLOCK
    smem = pl.BlockSpec(memory_space=pltpu.SMEM)
    vmem = pl.BlockSpec(memory_space=pltpu.VMEM)
    return pl.pallas_call(
        functools.partial(mass_kernel, scale=scale),
        out_shape=jax.ShapeDtypeStruct((blocks, 8, BLOCK), jnp.float32),
        in_specs=[smem, smem, smem, vmem, vmem],
        out_specs=vmem,
        scratch_shapes=[
            pltpu.VMEM((tokens, size), jnp.bfloat16),
            pltpu.VMEM((tokens // CHUNK, CHUNK, CHUNK), jnp.float32),
            pltpu.VMEM((blocks, 8, BLOCK), jnp.float32),
            pltpu.VMEM((CHUNK, BLOCK), jnp.float32),
        ],
        compiler_params=pltpu.CompilerParams(vmem_limit_bytes=24 * 1024 * 1024),
        cost_estimate=pl.CostEstimate(
            flops=2 * tokens * tokens * size, bytes_accessed=4 * tokens * size, transcendentals=tokens * tokens // 2
        ),
        name="head_mass",
    )(order, where, limit, q_rows, k_rows)


def exchanged(array, axis):
    return lax.all_to_all(array, axis, 0, 0, tiled=True)


def on_device(queries, keys, values, lengths, block_pos, w_in, b_in, output_weight, output_bias):
    q_rows = queries[0]
    k_rows = keys[0]
    v_rows = values[0]
    rows = q_rows.shape[0]
    seq = lax.axis_size("seq")
    batch = lax.axis_size("batch")
    heads_kv = output_weight.shape[1]
    hidden = output_weight.shape[0]
    head_size = k_rows.shape[1] // heads_kv
    group = q_rows.shape[1] // k_rows.shape[1]
    heads = heads_kv * group
    total = rows * seq
    order = block_pos[0]
    offsets = jnp.arange(rows, dtype=jnp.int32)
    mine = lax.axis_index("seq")
    query_pos = lax.dynamic_index_in_dim(order, mine, 0, keepdims=False) * rows + offsets
    limit = lengths[0]
    query_live = (query_pos < limit).astype(jnp.float32)
    where = jnp.sum(
        jnp.where(order[None, :] == jnp.arange(seq, dtype=jnp.int32)[:, None], jnp.arange(seq, dtype=jnp.int32)[None, :], 0),
        axis=1,
    ).astype(jnp.int32)

    by_head = jnp.moveaxis(q_rows.reshape(rows, heads, head_size), 1, 0)
    keys_by_head = jnp.moveaxis(k_rows.reshape(rows, heads_kv, head_size), 1, 0)
    keys_by_head = jnp.broadcast_to(keys_by_head[:, None], (heads_kv, group, rows, head_size)).reshape(
        heads, rows, head_size
    )
    both = exchanged(jnp.stack([by_head, keys_by_head], axis=1), "seq")
    own_q = both[:, 0].reshape(total, head_size)
    own_k = both[:, 1].reshape(total, head_size)
    partial = head_mass(order, where, lengths, own_q, own_k, 1.0 / math.sqrt(head_size))

    features = jnp.concatenate([q_rows, k_rows, v_rows], axis=1)
    width = features.shape[1] // seq
    spread = exchanged(jnp.moveaxis(features.reshape(rows, seq, width), 1, 0), "seq").reshape(total, width)

    pre = jnp.dot(features, w_in, preferred_element_type=jnp.float32) + b_in
    act = jax.nn.silu(pre).astype(jnp.bfloat16)
    pred = jnp.dot(act, output_weight, preferred_element_type=jnp.float32) + output_bias

    arrived = exchanged(partial, "seq")
    mass = jnp.sum(arrived.reshape(heads_kv, group * 8, rows), axis=1)
    labels = jnp.log1p(mass).T
    norm = 1.0 / math.sqrt(batch * total)
    resid = ((pred - labels) * query_live[:, None] * norm).astype(jnp.bfloat16)
    back = lax.dot_general(
        resid, output_weight, (((1,), (1,)), ((), ())), preferred_element_type=jnp.float32
    )
    sig = jax.nn.sigmoid(pre)
    delta = (back * sig * (1.0 + pre * (1.0 - sig))).astype(jnp.bfloat16)
    out_term = lax.dot_general(
        act, resid, (((0,), (0,)), ((), ())), preferred_element_type=jnp.float32
    )
    small = jnp.concatenate(
        [
            jnp.sum(delta.astype(jnp.float32), axis=0),
            out_term.ravel(),
            jnp.sum(resid.astype(jnp.float32), axis=0),
        ]
    )
    size = small.shape[0]
    piece = -(-size // (seq * 128)) * 128
    small = jnp.pad(small, (0, seq * piece - size)).reshape(seq, piece)
    small = jnp.sum(exchanged(small, "seq"), axis=0)
    small = exchanged(jnp.broadcast_to(small[None], (seq * batch, piece)), ("seq", "batch"))
    small = jnp.sum(small.reshape(seq, batch, piece), axis=1).ravel()
    grad_b_in = small[:hidden]
    output_weight_gradient = small[hidden : hidden + hidden * heads_kv].reshape(hidden, heads_kv)
    output_bias_gradient = small[hidden + hidden * heads_kv : size]

    every_delta = lax.all_gather(delta, "seq", axis=0, tiled=True)
    block = lax.dot_general(
        spread, every_delta, (((0,), (0,)), ((), ())), preferred_element_type=jnp.float32
    )
    block = block.reshape(batch, width // batch, hidden)
    grad_w_in = jnp.sum(exchanged(block, "batch"), axis=0)
    return (grad_w_in, grad_b_in, output_weight_gradient, output_bias_gradient)


def solution(mesh):
    return jax.shard_map(
        on_device,
        mesh=mesh,
        in_specs=(
            P("batch", "seq", None),
            P("batch", "seq", None),
            P("batch", "seq", None),
            P("batch"),
            P("batch", None),
            P(),
            P(),
            P(),
            P(),
        ),
        out_specs=(P(("seq", "batch"), None), P(), P(), P()),
        check_vma=False,
    )
```

```python
import functools
import math

import jax
import jax.numpy as jnp
from jax import lax
from jax.experimental import pallas as pl
from jax.experimental.pallas import tpu as pltpu
from jax.sharding import Mesh
from jax.sharding import PartitionSpec as P

BLOCK = 128
QUERIES = 512
KEYS = 512


def mass_kernel(order_ref, where_ref, limit_ref, q_ref, k_ref, out_ref, keys, scores, col, *, scale):
    blocks = q_ref.shape[0] // BLOCK
    limit = limit_ref[0]
    factor = scale * math.log2(math.e)
    diagonal = QUERIES // KEYS
    lanes = QUERIES // BLOCK

    def by_position(p, carry):
        start = pl.multiple_of(where_ref[p] * BLOCK, BLOCK)
        keys[pl.ds(pl.multiple_of(p * BLOCK, BLOCK), BLOCK), :] = k_ref[pl.ds(start, BLOCK), :]
        return carry

    lax.fori_loop(0, blocks, by_position, 0)
    col[...] = jnp.zeros_like(col)
    key = lax.broadcasted_iota(jnp.int32, (KEYS, QUERIES), 0)
    query = lax.broadcasted_iota(jnp.int32, (KEYS, QUERIES), 1)

    def folded(tile, op):
        return op(tile.reshape(KEYS // 8, 8, QUERIES), axis=0)

    def column_step(c, slot, weight):
        tile = scores[slot, c] * weight
        part = tile[:, :BLOCK]
        for i in range(1, lanes):
            part = part + tile[:, i * BLOCK : (i + 1) * BLOCK]
        col[c] += part

    def query_block(r, weight):
        parts = [
            q_ref[pl.ds(pl.multiple_of(where_ref[r * lanes + i] * BLOCK, BLOCK), BLOCK), :] for i in range(lanes)
        ]
        q_rows = jnp.concatenate(parts, axis=0)
        slot = lax.rem(r, 2)

        def product(c):
            k_rows = keys[pl.ds(pl.multiple_of(c * KEYS, KEYS), KEYS), :]
            return (
                lax.dot_general(k_rows, q_rows, (((1,), (1,)), ((), ())), preferred_element_type=jnp.float32)
                * factor
            )

        high = jnp.full((8, QUERIES), -1e30, jnp.float32)
        for d in range(diagonal):
            c = r * diagonal + d
            allowed = (key + d * KEYS <= query) & (key + c * KEYS < limit)
            tile = jnp.where(allowed, product(c), -1e30)
            scores[slot, c] = tile
            high = jnp.maximum(high, folded(tile, jnp.max))

        def score_step(c, high):
            tile = product(c)
            scores[slot, c] = tile
            column_step(c, 1 - slot, weight)
            return jnp.maximum(high, folded(tile, jnp.max))

        high = lax.fori_loop(0, r * diagonal, score_step, high)
        top = jnp.max(high, axis=0, keepdims=True)

        def exp_step(c, sums):
            tile = jnp.exp2(scores[slot, c] - top)
            scores[slot, c] = tile
            return sums + folded(tile, jnp.sum)

        sums = lax.fori_loop(0, (r + 1) * diagonal, exp_step, jnp.zeros((8, QUERIES), jnp.float32))
        total = jnp.sum(sums, axis=0, keepdims=True)
        live = lax.broadcasted_iota(jnp.int32, (1, QUERIES), 1) + r * QUERIES < limit
        return jnp.where(live, 1.0 / total, 0.0)

    count = (limit + QUERIES - 1) // QUERIES
    weight = lax.fori_loop(0, count, query_block, jnp.zeros((1, QUERIES), jnp.float32))
    last = lax.rem(count - 1, 2)

    def last_step(c, carry):
        column_step(c, last, weight)
        return carry

    lax.fori_loop(0, count * diagonal, last_step, 0)

    def store(i, carry):
        p = order_ref[i]
        per = KEYS // BLOCK
        own = col[p // per, pl.ds(pl.multiple_of(lax.rem(p, per) * BLOCK, BLOCK), BLOCK), :]
        out_ref[pl.ds(i, 1), :] = jnp.sum(own.T, axis=0, keepdims=True)
        return carry

    lax.fori_loop(0, blocks, store, 0)


def head_mass(order, where, limit, q_rows, k_rows, scale):
    tokens, size = q_rows.shape
    smem = pl.BlockSpec(memory_space=pltpu.SMEM)
    vmem = pl.BlockSpec(memory_space=pltpu.VMEM)
    return pl.pallas_call(
        functools.partial(mass_kernel, scale=scale),
        out_shape=jax.ShapeDtypeStruct((tokens // BLOCK, BLOCK), jnp.float32),
        in_specs=[smem, smem, smem, vmem, vmem],
        out_specs=vmem,
        scratch_shapes=[
            pltpu.VMEM((tokens, size), jnp.bfloat16),
            pltpu.VMEM((2, tokens // KEYS, KEYS, QUERIES), jnp.float32),
            pltpu.VMEM((tokens // KEYS, KEYS, BLOCK), jnp.float32),
        ],
        compiler_params=pltpu.CompilerParams(vmem_limit_bytes=48 * 1024 * 1024),
        cost_estimate=pl.CostEstimate(
            flops=2 * tokens * tokens * size, bytes_accessed=4 * tokens * size, transcendentals=tokens * tokens // 2
        ),
        name="head_mass",
    )(order, where, limit, q_rows, k_rows)


SEQ = ("y", "z", "core")
PLANE = ("y", "z")
SIDE = 4


def exchanged(array, axis):
    return lax.all_to_all(array, axis, 0, 0, tiled=True)


def shifted(array, axis, by):
    size = lax.axis_size(axis)
    return lax.ppermute(array, axis, [(i, (i + by) % size) for i in range(size)])


def summed(block, axis):
    size = lax.axis_size(axis)
    me = lax.axis_index(axis)
    total = lax.dynamic_index_in_dim(block, me, 0, keepdims=False)
    for by in range(1, size):
        part = lax.dynamic_index_in_dim(block, lax.rem(me + by, size), 0, keepdims=False)
        total = total + shifted(part, axis, by)
    return total


def in_three(array):
    high = lax.reduce_precision(array, 8, 7)
    middle = lax.reduce_precision(array - high, 8, 7)
    low = array - high - middle
    return jnp.concatenate([high, middle, low], axis=-1).astype(jnp.bfloat16)


def from_three(parts):
    wide = parts.astype(jnp.float32)
    size = wide.shape[-1] // 3
    return wide[..., :size] + wide[..., size : 2 * size] + wide[..., 2 * size :]


def on_device(queries, keys, values, lengths, block_pos, w_in, b_in, output_weight, output_bias):
    q_rows = queries[0]
    k_rows = keys[0]
    v_rows = values[0]
    rows = q_rows.shape[0]
    seq = lax.axis_size(SEQ)
    chips = lax.axis_size(PLANE)
    cores = lax.axis_size("core")
    batch = lax.axis_size("batch")
    heads_kv = output_weight.shape[1]
    hidden = output_weight.shape[0]
    head_size = k_rows.shape[1] // heads_kv
    group = q_rows.shape[1] // k_rows.shape[1]
    heads = heads_kv * group
    total = rows * seq
    order = block_pos[0]
    limit = lengths[0]
    places = jnp.arange(seq, dtype=jnp.int32)
    where = jnp.sum(jnp.where(order[None, :] == places[:, None], places[None, :], 0), axis=1).astype(jnp.int32)
    chip = lax.axis_index(PLANE)
    core = lax.axis_index("core")

    by_head = jnp.moveaxis(q_rows.reshape(rows, heads, head_size), 1, 0)
    keys_by_head = jnp.moveaxis(k_rows.reshape(rows, heads_kv, head_size), 1, 0)
    keys_by_head = jnp.broadcast_to(keys_by_head[:, None], (heads_kv, group, rows, head_size)).reshape(
        heads, rows, head_size
    )
    both = exchanged(jnp.stack([by_head, keys_by_head], axis=1), SEQ)

    features = jnp.concatenate([q_rows, k_rows, v_rows], axis=1)
    pre = jnp.dot(features, w_in, preferred_element_type=jnp.float32) + b_in
    sig = jax.nn.sigmoid(pre)
    act = (pre * sig).astype(jnp.bfloat16)
    pred = jnp.dot(act, output_weight, preferred_element_type=jnp.float32) + output_bias
    slope = sig * (1.0 + pre * (1.0 - sig))
    largest = jnp.maximum(jnp.max(jnp.abs(slope), axis=1, keepdims=True), 1e-30)
    slope = (slope / largest).astype(jnp.float16)

    width = features.shape[1] // chips
    part = hidden // chips
    carried = jnp.concatenate(
        [
            features.reshape(rows, chips, width),
            act.reshape(rows, chips, part),
            jnp.broadcast_to(
                jnp.pad(
                    jnp.concatenate([in_three(pred), in_three(largest)], axis=1), ((0, 0), (0, part - 3 * heads_kv - 3))
                )[:, None],
                (rows, chips, part),
            ),
        ],
        axis=2,
    )
    own_q = both[:, 0].reshape(total, head_size)
    own_k = both[:, 1].reshape(total, head_size)
    own_q, own_k, slope, carried = lax.optimization_barrier((own_q, own_k, slope, jnp.moveaxis(carried, 1, 0)))
    spread = exchanged(carried, PLANE)
    partial = head_mass(order, where, lengths, own_q, own_k, 1.0 / math.sqrt(head_size))

    to_cores = jnp.moveaxis(partial.reshape(chips, cores, rows), 1, 0)
    to_all = jnp.broadcast_to(to_cores[None], (chips, cores, chips, rows)).reshape(seq, chips, rows)
    slope, to_all = lax.optimization_barrier((slope, to_all))
    arrived = exchanged(to_all, SEQ)
    slopes = lax.all_gather(slope, PLANE, axis=0, tiled=True)
    slopes, arrived = lax.optimization_barrier((slopes, arrived))
    mass = jnp.sum(arrived.reshape(heads_kv, group, chips * rows), axis=1)
    labels = jnp.log1p(mass).T

    spread = spread.reshape(chips * rows, width + 2 * part)
    feats = spread[:, :width]
    acts = spread[:, width : width + part]
    predicted = from_three(spread[:, width + part : width + part + 3 * heads_kv])
    factor = from_three(spread[:, width + part + 3 * heads_kv : width + part + 3 * heads_kv + 3])
    offsets = jnp.arange(rows, dtype=jnp.int32)
    blocks = lax.dynamic_index_in_dim(order.reshape(chips, cores), core, 1, keepdims=False)
    position = (blocks[:, None] * rows + offsets[None, :]).reshape(-1)
    live = (position < limit).astype(jnp.float32)
    norm = 1.0 / math.sqrt(batch * total)
    resid = ((predicted - labels) * live[:, None] * norm).astype(jnp.bfloat16)
    back = lax.dot_general(
        resid, output_weight, (((1,), (1,)), ((), ())), preferred_element_type=jnp.float32
    )
    delta = (back * (slopes.astype(jnp.float32) * factor)).astype(jnp.bfloat16)
    block = lax.dot_general(
        feats, delta, (((0,), (0,)), ((), ())), preferred_element_type=jnp.float32
    )
    block = summed(block.reshape(cores, width // cores, hidden), "core")

    out_part = lax.dot_general(acts, resid, (((0,), (0,)), ((), ())), preferred_element_type=jnp.float32)
    b_part = lax.dynamic_index_in_dim(
        jnp.sum(delta.astype(jnp.float32), axis=0).reshape(chips, part), chip, 0, keepdims=False
    )
    small = jnp.concatenate([out_part.ravel(), b_part, jnp.sum(resid.astype(jnp.float32), axis=0)])
    size = small.shape[0]
    small = jnp.pad(small, (0, -size % 128))
    small = exchanged(jnp.broadcast_to(small[None], (seq, small.shape[0])), SEQ)
    small = jnp.sum(small.reshape(chips, cores, small.shape[1]), axis=1)
    across = small.shape[1]
    small = jnp.pad(small.ravel(), (0, -small.size % hidden)).reshape(-1, hidden)
    block = block.reshape(batch, width // (cores * batch), hidden)
    ending = jnp.concatenate([block, jnp.broadcast_to(small[None], (batch, *small.shape))], axis=1)
    ending = summed(ending, "batch")
    grad_w_in = ending[: block.shape[1]]
    small = ending[block.shape[1] :].ravel()[: chips * across].reshape(chips, across)
    output_weight_gradient = small[:, : part * heads_kv].reshape(hidden, heads_kv)
    grad_b_in = small[:, part * heads_kv : part * heads_kv + part].reshape(hidden)
    output_bias_gradient = small[0, part * heads_kv + part : size]
    return (grad_w_in, grad_b_in, output_weight_gradient, output_bias_gradient)


def solution(mesh):
    cores = mesh.shape["seq"] // (SIDE * SIDE)
    fine = Mesh(
        mesh.devices.reshape(SIDE, SIDE, cores, mesh.shape["batch"]), SEQ + ("batch",)
    )
    return jax.shard_map(
        on_device,
        mesh=fine,
        in_specs=(
            P("batch", SEQ, None),
            P("batch", SEQ, None),
            P("batch", SEQ, None),
            P("batch"),
            P("batch", None),
            P(),
            P(),
            P(),
            P(),
        ),
        out_specs=(P(SEQ + ("batch",), None), P(), P(), P()),
        check_vma=False,
    )
```

```python
import functools
import math

import jax
import jax.numpy as jnp
from jax import lax
from jax.experimental import pallas as pl
from jax.experimental.pallas import tpu as pltpu
from jax.sharding import Mesh
from jax.sharding import PartitionSpec as P

BLOCK = 128
QUERIES = 512
KEYS = 512


def mass_kernel(order_ref, limit_ref, both_ref, out_ref, where_ref, keys, scores, col, *, scale):
    blocks = both_ref.shape[0]
    limit = limit_ref[0]
    factor = scale * math.log2(math.e)
    diagonal = QUERIES // KEYS
    lanes = QUERIES // BLOCK

    def by_position(i, carry):
        p = order_ref[i]
        where_ref[p] = i
        keys[pl.ds(pl.multiple_of(p * BLOCK, BLOCK), BLOCK), :] = both_ref[i, 1]
        return carry

    lax.fori_loop(0, blocks, by_position, 0)
    col[...] = jnp.zeros_like(col)
    key = lax.broadcasted_iota(jnp.int32, (KEYS, QUERIES), 0)
    query = lax.broadcasted_iota(jnp.int32, (KEYS, QUERIES), 1)

    def folded(tile, op):
        return op(tile.reshape(KEYS // 8, 8, QUERIES), axis=0)

    def column_step(c, slot, weight):
        tile = scores[slot, c] * weight
        part = tile[:, :BLOCK]
        for i in range(1, lanes):
            part = part + tile[:, i * BLOCK : (i + 1) * BLOCK]
        col[c] += part

    def query_block(r, weight):
        parts = [both_ref[where_ref[r * lanes + i], 0] for i in range(lanes)]
        q_rows = jnp.concatenate(parts, axis=0)
        slot = lax.rem(r, 2)

        def product(c):
            k_rows = keys[pl.ds(pl.multiple_of(c * KEYS, KEYS), KEYS), :]
            return (
                lax.dot_general(k_rows, q_rows, (((1,), (1,)), ((), ())), preferred_element_type=jnp.float32)
                * factor
            )

        high = jnp.full((8, QUERIES), -1e30, jnp.float32)
        for d in range(diagonal):
            c = r * diagonal + d
            allowed = (key + d * KEYS <= query) & (key + c * KEYS < limit)
            tile = jnp.where(allowed, product(c), -1e30)
            scores[slot, c] = tile
            high = jnp.maximum(high, folded(tile, jnp.max))

        def score_step(c, high):
            tile = product(c)
            scores[slot, c] = tile
            column_step(c, 1 - slot, weight)
            return jnp.maximum(high, folded(tile, jnp.max))

        high = lax.fori_loop(0, r * diagonal, score_step, high)
        top = jnp.max(high, axis=0, keepdims=True)

        def exp_step(c, sums):
            tile = jnp.exp2(scores[slot, c] - top)
            scores[slot, c] = tile
            return sums + folded(tile, jnp.sum)

        sums = lax.fori_loop(0, (r + 1) * diagonal, exp_step, jnp.zeros((8, QUERIES), jnp.float32))
        total = jnp.sum(sums, axis=0, keepdims=True)
        live = lax.broadcasted_iota(jnp.int32, (1, QUERIES), 1) + r * QUERIES < limit
        return jnp.where(live, 1.0 / total, 0.0)

    count = (limit + QUERIES - 1) // QUERIES
    weight = lax.fori_loop(0, count, query_block, jnp.zeros((1, QUERIES), jnp.float32))
    last = lax.rem(count - 1, 2)

    def last_step(c, carry):
        column_step(c, last, weight)
        return carry

    lax.fori_loop(0, count * diagonal, last_step, 0)

    def store(i, carry):
        p = order_ref[i]
        per = KEYS // BLOCK
        own = col[p // per, pl.ds(pl.multiple_of(lax.rem(p, per) * BLOCK, BLOCK), BLOCK), :]
        out_ref[pl.ds(i, 1), :] = jnp.sum(own.T, axis=0, keepdims=True)
        return carry

    lax.fori_loop(0, blocks, store, 0)


def head_mass(order, limit, both, scale):
    blocks, _, rows, size = both.shape
    tokens = blocks * rows
    smem = pl.BlockSpec(memory_space=pltpu.SMEM)
    vmem = pl.BlockSpec(memory_space=pltpu.VMEM)
    return pl.pallas_call(
        functools.partial(mass_kernel, scale=scale),
        out_shape=jax.ShapeDtypeStruct((blocks, BLOCK), jnp.float32),
        in_specs=[smem, smem, vmem],
        out_specs=vmem,
        scratch_shapes=[
            pltpu.SMEM((blocks,), jnp.int32),
            pltpu.VMEM((tokens, size), jnp.bfloat16),
            pltpu.VMEM((2, tokens // KEYS, KEYS, QUERIES), jnp.float32),
            pltpu.VMEM((tokens // KEYS, KEYS, BLOCK), jnp.float32),
        ],
        compiler_params=pltpu.CompilerParams(vmem_limit_bytes=48 * 1024 * 1024),
        cost_estimate=pl.CostEstimate(
            flops=2 * tokens * tokens * size, bytes_accessed=4 * tokens * size, transcendentals=tokens * tokens // 2
        ),
        name="head_mass",
    )(order, limit, both)


def by_head_kernel(q_ref, k_ref, out_ref):
    heads, _, _, size = out_ref.shape
    group = q_ref.shape[1] // k_ref.shape[1]
    for h in range(heads):
        g = h // group
        out_ref[h, 0] = q_ref[:, h * size : (h + 1) * size]
        out_ref[h, 1] = k_ref[:, g * size : (g + 1) * size]


def by_head(q_rows, k_rows, size):
    rows, width = q_rows.shape
    vmem = pl.BlockSpec(memory_space=pltpu.VMEM)
    return pl.pallas_call(
        by_head_kernel,
        out_shape=jax.ShapeDtypeStruct((width // size, 2, rows, size), q_rows.dtype),
        in_specs=[vmem, vmem],
        out_specs=vmem,
        compiler_params=pltpu.CompilerParams(vmem_limit_bytes=16 * 1024 * 1024),
        name="by_head",
    )(q_rows, k_rows)


SEQ = ("y", "z", "core")
PLANE = ("y", "z")
SIDE = 4


def exchanged(array, axis):
    return lax.all_to_all(array, axis, 0, 0, tiled=True)


def shifted(array, axis, by):
    size = lax.axis_size(axis)
    return lax.ppermute(array, axis, [(i, (i + by) % size) for i in range(size)])


def summed(block, axis):
    size = lax.axis_size(axis)
    me = lax.axis_index(axis)
    total = lax.dynamic_index_in_dim(block, me, 0, keepdims=False)
    for by in range(1, size):
        part = lax.dynamic_index_in_dim(block, lax.rem(me + by, size), 0, keepdims=False)
        total = total + shifted(part, axis, by)
    return total


def in_three(array):
    high = lax.reduce_precision(array, 8, 7)
    middle = lax.reduce_precision(array - high, 8, 7)
    low = array - high - middle
    return jnp.concatenate([high, middle, low], axis=-1).astype(jnp.bfloat16)


def from_three(parts):
    wide = parts.astype(jnp.float32)
    size = wide.shape[-1] // 3
    return wide[..., :size] + wide[..., size : 2 * size] + wide[..., 2 * size :]


def on_device(queries, keys, values, lengths, block_pos, w_in, b_in, output_weight, output_bias):
    q_rows = queries[0]
    k_rows = keys[0]
    v_rows = values[0]
    rows = q_rows.shape[0]
    seq = lax.axis_size(SEQ)
    chips = lax.axis_size(PLANE)
    cores = lax.axis_size("core")
    batch = lax.axis_size("batch")
    heads_kv = output_weight.shape[1]
    hidden = output_weight.shape[0]
    head_size = k_rows.shape[1] // heads_kv
    group = q_rows.shape[1] // k_rows.shape[1]
    total = rows * seq
    order = block_pos[0]
    limit = lengths[0]
    chip = lax.axis_index(PLANE)
    core = lax.axis_index("core")

    both = exchanged(by_head(q_rows, k_rows, head_size), SEQ)

    features = jnp.concatenate([q_rows, k_rows, v_rows], axis=1)
    pre = jnp.dot(features, w_in, preferred_element_type=jnp.float32) + b_in
    sig = jax.nn.sigmoid(pre)
    act = (pre * sig).astype(jnp.bfloat16)
    pred = jnp.dot(act, output_weight, preferred_element_type=jnp.float32) + output_bias
    slope = sig * (1.0 + pre * (1.0 - sig))
    largest = jnp.maximum(jnp.max(jnp.abs(slope), axis=1, keepdims=True), 1e-30)
    slope = (slope / largest).astype(jnp.float16)

    width = features.shape[1] // chips
    part = hidden // chips
    carried = jnp.concatenate(
        [
            features.reshape(rows, chips, width),
            act.reshape(rows, chips, part),
            jnp.broadcast_to(
                jnp.pad(
                    jnp.concatenate([in_three(pred), in_three(largest)], axis=1), ((0, 0), (0, part - 3 * heads_kv - 3))
                )[:, None],
                (rows, chips, part),
            ),
        ],
        axis=2,
    )
    both, slope, carried = lax.optimization_barrier((both, slope, jnp.moveaxis(carried, 1, 0)))
    spread = exchanged(carried, PLANE)
    partial = head_mass(order, lengths, both, 1.0 / math.sqrt(head_size))

    to_cores = jnp.moveaxis(partial.reshape(chips, cores, rows), 1, 0)
    to_all = jnp.broadcast_to(to_cores[None], (chips, cores, chips, rows)).reshape(seq, chips, rows)
    slope, to_all = lax.optimization_barrier((slope, to_all))
    arrived = exchanged(to_all, SEQ)
    slopes = lax.all_gather(slope, PLANE, axis=0, tiled=True)
    slopes, arrived = lax.optimization_barrier((slopes, arrived))
    mass = jnp.sum(arrived.reshape(heads_kv, group, chips * rows), axis=1)
    labels = jnp.log1p(mass).T

    spread = spread.reshape(chips * rows, width + 2 * part)
    feats = spread[:, :width]
    acts = spread[:, width : width + part]
    predicted = from_three(spread[:, width + part : width + part + 3 * heads_kv])
    factor = from_three(spread[:, width + part + 3 * heads_kv : width + part + 3 * heads_kv + 3])
    offsets = jnp.arange(rows, dtype=jnp.int32)
    blocks = lax.dynamic_index_in_dim(order.reshape(chips, cores), core, 1, keepdims=False)
    position = (blocks[:, None] * rows + offsets[None, :]).reshape(-1)
    live = (position < limit).astype(jnp.float32)
    norm = 1.0 / math.sqrt(batch * total)
    resid = ((predicted - labels) * live[:, None] * norm).astype(jnp.bfloat16)
    back = lax.dot_general(
        resid, output_weight, (((1,), (1,)), ((), ())), preferred_element_type=jnp.float32
    )
    delta = (back * (slopes.astype(jnp.float32) * factor)).astype(jnp.bfloat16)
    out_part = lax.dot_general(acts, resid, (((0,), (0,)), ((), ())), preferred_element_type=jnp.float32)
    b_part = lax.dynamic_index_in_dim(
        jnp.sum(delta.astype(jnp.float32), axis=0).reshape(chips, part), chip, 0, keepdims=False
    )
    small = jnp.concatenate([out_part.ravel(), b_part, jnp.sum(resid.astype(jnp.float32), axis=0)])
    size = small.shape[0]
    small = jnp.pad(small, (0, -size % 128))
    small = exchanged(jnp.broadcast_to(small[None], (seq, small.shape[0])), SEQ)
    block = lax.dot_general(
        feats, delta, (((0,), (0,)), ((), ())), preferred_element_type=jnp.float32
    )
    block = summed(block.reshape(cores, width // cores, hidden), "core")
    grad_w_in = summed(block.reshape(batch, width // (cores * batch), hidden), "batch")
    small = jnp.sum(small.reshape(chips, cores, small.shape[1]), axis=1)
    small = small + sum(shifted(small, "batch", by) for by in range(1, batch))
    output_weight_gradient = small[:, : part * heads_kv].reshape(hidden, heads_kv)
    grad_b_in = small[:, part * heads_kv : part * heads_kv + part].reshape(hidden)
    output_bias_gradient = small[0, part * heads_kv + part : size]
    return (grad_w_in, grad_b_in, output_weight_gradient, output_bias_gradient)


def solution(mesh):
    cores = mesh.shape["seq"] // (SIDE * SIDE)
    fine = Mesh(
        mesh.devices.reshape(SIDE, SIDE, cores, mesh.shape["batch"]), SEQ + ("batch",)
    )
    return jax.shard_map(
        on_device,
        mesh=fine,
        in_specs=(
            P("batch", SEQ, None),
            P("batch", SEQ, None),
            P("batch", SEQ, None),
            P("batch"),
            P("batch", None),
            P(),
            P(),
            P(),
            P(),
        ),
        out_specs=(P(SEQ + ("batch",), None), P(), P(), P()),
        check_vma=False,
    )
```

```python
import functools
import math

import jax
import jax.numpy as jnp
from jax import lax
from jax.experimental import pallas as pl
from jax.experimental.pallas import tpu as pltpu
from jax.sharding import Mesh
from jax.sharding import PartitionSpec as P

BLOCK = 128
QUERIES = 512
KEYS = 512


def mass_kernel(order_ref, limit_ref, both_ref, out_ref, where_ref, keys, scores, col, *, scale):
    blocks = both_ref.shape[0]
    limit = limit_ref[0]
    factor = scale * math.log2(math.e)
    diagonal = QUERIES // KEYS
    lanes = QUERIES // BLOCK

    def by_position(i, carry):
        p = order_ref[i]
        where_ref[p] = i
        keys[pl.ds(pl.multiple_of(p * BLOCK, BLOCK), BLOCK), :] = both_ref[i, 1]
        return carry

    lax.fori_loop(0, blocks, by_position, 0)
    col[...] = jnp.zeros_like(col)
    key = lax.broadcasted_iota(jnp.int32, (KEYS, QUERIES), 0)
    query = lax.broadcasted_iota(jnp.int32, (KEYS, QUERIES), 1)

    def folded(tile, op):
        return op(tile.reshape(KEYS // 8, 8, QUERIES), axis=0)

    def column_step(c, slot, weight):
        tile = scores[slot, c] * weight
        part = tile[:, :BLOCK]
        for i in range(1, lanes):
            part = part + tile[:, i * BLOCK : (i + 1) * BLOCK]
        col[c] += part

    def query_block(r, weight):
        parts = [both_ref[where_ref[r * lanes + i], 0] for i in range(lanes)]
        q_rows = jnp.concatenate(parts, axis=0)
        slot = lax.rem(r, 2)

        def product(c):
            k_rows = keys[pl.ds(pl.multiple_of(c * KEYS, KEYS), KEYS), :]
            return (
                lax.dot_general(k_rows, q_rows, (((1,), (1,)), ((), ())), preferred_element_type=jnp.float32)
                * factor
            )

        high = jnp.full((8, QUERIES), -1e30, jnp.float32)
        for d in range(diagonal):
            c = r * diagonal + d
            allowed = (key + d * KEYS <= query) & (key + c * KEYS < limit)
            tile = jnp.where(allowed, product(c), -1e30)
            scores[slot, c] = tile
            high = jnp.maximum(high, folded(tile, jnp.max))

        def score_step(c, high):
            column_step(c, 1 - slot, weight)
            tile = product(c)
            scores[slot, c] = tile
            return jnp.maximum(high, folded(tile, jnp.max))

        high = lax.fori_loop(0, r * diagonal, score_step, high)
        top = jnp.max(high, axis=0, keepdims=True)

        def exp_step(c, sums):
            tile = jnp.exp2(scores[slot, c] - top)
            scores[slot, c] = tile
            return sums + folded(tile, jnp.sum)

        sums = lax.fori_loop(0, (r + 1) * diagonal, exp_step, jnp.zeros((8, QUERIES), jnp.float32))
        total = jnp.sum(sums, axis=0, keepdims=True)
        live = lax.broadcasted_iota(jnp.int32, (1, QUERIES), 1) + r * QUERIES < limit
        return jnp.where(live, 1.0 / total, 0.0)

    count = (limit + QUERIES - 1) // QUERIES
    weight = lax.fori_loop(0, count, query_block, jnp.zeros((1, QUERIES), jnp.float32))
    last = lax.rem(count - 1, 2)

    def last_step(c, carry):
        column_step(c, last, weight)
        return carry

    lax.fori_loop(0, count * diagonal, last_step, 0)

    def store(i, carry):
        p = order_ref[i]
        per = KEYS // BLOCK
        own = col[p // per, pl.ds(pl.multiple_of(lax.rem(p, per) * BLOCK, BLOCK), BLOCK), :]
        out_ref[pl.ds(i, 1), :] = jnp.sum(own.T, axis=0, keepdims=True)
        return carry

    lax.fori_loop(0, blocks, store, 0)


def head_mass(order, limit, both, scale):
    blocks, _, rows, size = both.shape
    tokens = blocks * rows
    smem = pl.BlockSpec(memory_space=pltpu.SMEM)
    vmem = pl.BlockSpec(memory_space=pltpu.VMEM)
    return pl.pallas_call(
        functools.partial(mass_kernel, scale=scale),
        out_shape=jax.ShapeDtypeStruct((blocks, BLOCK), jnp.float32),
        in_specs=[smem, smem, vmem],
        out_specs=vmem,
        scratch_shapes=[
            pltpu.SMEM((blocks,), jnp.int32),
            pltpu.VMEM((tokens, size), jnp.bfloat16),
            pltpu.VMEM((2, tokens // KEYS, KEYS, QUERIES), jnp.float32),
            pltpu.VMEM((tokens // KEYS, KEYS, BLOCK), jnp.float32),
        ],
        compiler_params=pltpu.CompilerParams(vmem_limit_bytes=48 * 1024 * 1024),
        cost_estimate=pl.CostEstimate(
            flops=2 * tokens * tokens * size, bytes_accessed=4 * tokens * size, transcendentals=tokens * tokens // 2
        ),
        name="head_mass",
    )(order, limit, both)


def by_head_kernel(q_ref, k_ref, out_ref):
    heads, _, _, size = out_ref.shape
    group = q_ref.shape[1] // k_ref.shape[1]
    for h in range(heads):
        g = h // group
        out_ref[h, 0] = q_ref[:, h * size : (h + 1) * size]
        out_ref[h, 1] = k_ref[:, g * size : (g + 1) * size]


def by_head(q_rows, k_rows, size):
    rows, width = q_rows.shape
    vmem = pl.BlockSpec(memory_space=pltpu.VMEM)
    return pl.pallas_call(
        by_head_kernel,
        out_shape=jax.ShapeDtypeStruct((width // size, 2, rows, size), q_rows.dtype),
        in_specs=[vmem, vmem],
        out_specs=vmem,
        compiler_params=pltpu.CompilerParams(vmem_limit_bytes=16 * 1024 * 1024),
        name="by_head",
    )(q_rows, k_rows)


SEQ = ("y", "z", "core")
PLANE = ("y", "z")
SIDE = 4
FINER = 2048.0


def exchanged(array, axis):
    return lax.all_to_all(array, axis, 0, 0, tiled=True)


def shifted(array, axis, by):
    size = lax.axis_size(axis)
    return lax.ppermute(array, axis, [(i, (i + by) % size) for i in range(size)])


def summed(block, axis):
    size = lax.axis_size(axis)
    me = lax.axis_index(axis)
    total = lax.dynamic_index_in_dim(block, me, 0, keepdims=False)
    for by in range(1, size):
        part = lax.dynamic_index_in_dim(block, lax.rem(me + by, size), 0, keepdims=False)
        total = total + shifted(part, axis, by)
    return total


def beside(i):
    return i + 1 - 2 * (i % 2)


def across(i):
    return SIDE - 1 - i


def swapped(array, other):
    return lax.ppermute(array, "batch", [(i, other(i)) for i in range(SIDE)])


def halved(block, first, second):
    me = lax.axis_index("batch")

    def two(i):
        return jnp.stack([lax.dynamic_index_in_dim(block, j, 0, keepdims=False) for j in (i, second(i))])

    return two(me) + swapped(two(first(me)), first)


def finished(kept, second):
    return kept[0] + swapped(kept[1], second)


def in_three(array):
    high = lax.reduce_precision(array, 8, 7)
    middle = lax.reduce_precision(array - high, 8, 7)
    low = array - high - middle
    return jnp.concatenate([high, middle, low], axis=-1).astype(jnp.bfloat16)


def from_three(parts):
    wide = parts.astype(jnp.float32)
    size = wide.shape[-1] // 3
    return wide[..., :size] + wide[..., size : 2 * size] + wide[..., 2 * size :]


def on_device(queries, keys, values, lengths, block_pos, w_in, b_in, output_weight, output_bias):
    q_rows = queries[0]
    k_rows = keys[0]
    v_rows = values[0]
    rows = q_rows.shape[0]
    seq = lax.axis_size(SEQ)
    chips = lax.axis_size(PLANE)
    cores = lax.axis_size("core")
    batch = lax.axis_size("batch")
    heads_kv = output_weight.shape[1]
    hidden = output_weight.shape[0]
    head_size = k_rows.shape[1] // heads_kv
    total = rows * seq
    order = block_pos[0]
    limit = lengths[0]
    chip = lax.axis_index(PLANE)
    core = lax.axis_index("core")

    both = exchanged(by_head(q_rows, k_rows, head_size), SEQ)

    features = jnp.concatenate([q_rows, k_rows, v_rows], axis=1)
    pre = jnp.dot(features, w_in, preferred_element_type=jnp.float32) + b_in
    sig = jax.nn.sigmoid(pre)
    act = (pre * sig).astype(jnp.bfloat16)
    pred = jnp.dot(act, output_weight, preferred_element_type=jnp.float32) + output_bias
    slope = sig * (1.0 + pre * (1.0 - sig))
    largest = jnp.maximum(jnp.max(jnp.abs(slope), axis=1, keepdims=True), 1e-30)
    slope = (slope / largest).astype(jnp.float16)

    width = features.shape[1] // chips
    part = hidden // chips
    carried = jnp.concatenate(
        [
            features.reshape(rows, chips, width),
            act.reshape(rows, chips, part),
            jnp.broadcast_to(
                jnp.pad(
                    jnp.concatenate([in_three(pred), in_three(largest)], axis=1), ((0, 0), (0, part - 3 * heads_kv - 3))
                )[:, None],
                (rows, chips, part),
            ),
        ],
        axis=2,
    )
    both, slope, carried = lax.optimization_barrier((both, slope, jnp.moveaxis(carried, 1, 0)))
    spread = exchanged(carried, PLANE)
    partial = head_mass(order, lengths, both, 1.0 / math.sqrt(head_size))

    by_core = partial.reshape(chips, cores, rows)
    both_heads = lax.dynamic_index_in_dim(by_core, core, 1, keepdims=False)
    both_heads = both_heads + shifted(lax.dynamic_index_in_dim(by_core, 1 - core, 1, keepdims=False), "core", 1)
    high = lax.reduce_precision(both_heads, 5, 10)
    left = (both_heads - high) * FINER
    middle = lax.reduce_precision(left, 5, 10)
    low = (left - middle) * FINER
    carry = jnp.stack([high, middle, low]).astype(jnp.float16).reshape(-1, hidden)
    taken = carry.shape[0]
    carry = jnp.pad(carry, ((0, -taken % 16), (0, 0)))
    arrived = lax.all_gather(jnp.concatenate([slope, carry]), PLANE, axis=0, tiled=False)
    slopes = arrived.reshape(-1, hidden)
    padded = rows + carry.shape[0]
    sums = jnp.sum(
        arrived[:, rows:].astype(jnp.float32).reshape(heads_kv, chips // heads_kv, carry.shape[0], hidden), axis=1
    )
    third = taken // 3
    mass = sums[:, :third] + (sums[:, third : 2 * third] + sums[:, 2 * third : taken] * (1.0 / FINER)) * (1.0 / FINER)
    mass = jnp.pad(mass.reshape(heads_kv, chips, rows), ((0, 0), (0, 0), (0, padded - rows)))
    labels = jnp.log1p(mass.reshape(heads_kv, chips * padded)).T

    spread = jnp.pad(spread, ((0, 0), (0, padded - rows), (0, 0))).reshape(chips * padded, width + 2 * part)
    feats = spread[:, :width]
    acts = spread[:, width : width + part]
    predicted = from_three(spread[:, width + part : width + part + 3 * heads_kv])
    factor = from_three(spread[:, width + part + 3 * heads_kv : width + part + 3 * heads_kv + 3])
    offsets = jnp.arange(rows, dtype=jnp.int32)
    blocks = lax.dynamic_index_in_dim(order.reshape(chips, cores), core, 1, keepdims=False)
    position = (blocks[:, None] * rows + offsets[None, :]).reshape(-1)
    live = (position < limit).astype(jnp.float32)
    live = jnp.pad(live.reshape(chips, rows), ((0, 0), (0, padded - rows))).reshape(-1)
    norm = 1.0 / math.sqrt(batch * total)
    resid = ((predicted - labels) * live[:, None] * norm).astype(jnp.bfloat16)
    back = lax.dot_general(
        resid, output_weight, (((1,), (1,)), ((), ())), preferred_element_type=jnp.float32
    )
    delta = (back * (slopes.astype(jnp.float32) * factor)).astype(jnp.bfloat16)
    out_part = lax.dot_general(acts, resid, (((0,), (0,)), ((), ())), preferred_element_type=jnp.float32)
    b_part = lax.dynamic_index_in_dim(
        jnp.sum(delta.astype(jnp.float32), axis=0).reshape(chips, part), chip, 0, keepdims=False
    )
    small = jnp.concatenate([out_part.ravel(), b_part, jnp.sum(resid.astype(jnp.float32), axis=0)])
    size = small.shape[0]
    small = jnp.pad(small, (0, -size % 128))
    small = exchanged(jnp.broadcast_to(small[None], (seq, small.shape[0])), SEQ)
    block = lax.dot_general(
        feats, delta, (((0,), (0,)), ((), ())), preferred_element_type=jnp.float32
    )
    block = summed(block.reshape(cores, width // cores, hidden), "core")
    block = block.reshape(batch, width // (cores * batch), hidden)
    half = hidden // 2
    kept = [halved(block[:, :, :half], beside, across), halved(block[:, :, half:], across, beside)]
    grad_w_in = jnp.concatenate([finished(kept[0], across), finished(kept[1], beside)], axis=1)
    small = jnp.sum(small.reshape(chips, cores, small.shape[1]), axis=1)
    small = small + sum(shifted(small, "batch", by) for by in range(1, batch))
    output_weight_gradient = small[:, : part * heads_kv].reshape(hidden, heads_kv)
    grad_b_in = small[:, part * heads_kv : part * heads_kv + part].reshape(hidden)
    output_bias_gradient = small[0, part * heads_kv + part : size]
    return (grad_w_in, grad_b_in, output_weight_gradient, output_bias_gradient)


def solution(mesh):
    cores = mesh.shape["seq"] // (SIDE * SIDE)
    fine = Mesh(
        mesh.devices.reshape(SIDE, SIDE, cores, mesh.shape["batch"]), SEQ + ("batch",)
    )
    return jax.shard_map(
        on_device,
        mesh=fine,
        in_specs=(
            P("batch", SEQ, None),
            P("batch", SEQ, None),
            P("batch", SEQ, None),
            P("batch"),
            P("batch", None),
            P(),
            P(),
            P(),
            P(),
        ),
        out_specs=(P(SEQ + ("batch",), None), P(), P(), P()),
        check_vma=False,
    )
```

```python
import functools
import math

import jax
import jax.numpy as jnp
from jax import lax
from jax.experimental import pallas as pl
from jax.experimental.pallas import tpu as pltpu
from jax.sharding import Mesh
from jax.sharding import PartitionSpec as P

BLOCK = 128
QUERIES = 512
KEYS = 512


def mass_kernel(order_ref, limit_ref, both_ref, out_ref, where_ref, keys, even, odd, col, *, scale):
    blocks = both_ref.shape[0]
    limit = limit_ref[0]
    factor = scale * math.log2(math.e)
    diagonal = QUERIES // KEYS
    lanes = QUERIES // BLOCK

    def by_position(i, carry):
        p = order_ref[i]
        where_ref[p] = i
        keys[pl.ds(pl.multiple_of(p * BLOCK, BLOCK), BLOCK), :] = both_ref[i, 1]
        return carry

    lax.fori_loop(0, blocks, by_position, 0)
    col[...] = jnp.zeros_like(col)
    key = lax.broadcasted_iota(jnp.int32, (KEYS, QUERIES), 0)
    query = lax.broadcasted_iota(jnp.int32, (KEYS, QUERIES), 1)

    def folded(tile, op):
        return op(tile.reshape(KEYS // 8, 8, QUERIES), axis=0)

    def column_step(c, scores, weight):
        tile = scores[c] * weight
        part = tile[:, :BLOCK]
        for i in range(1, lanes):
            part = part + tile[:, i * BLOCK : (i + 1) * BLOCK]
        col[c] += part

    def columns(scores, weight, r):
        def one(c, carry):
            column_step(c, scores, weight)
            return carry

        lax.fori_loop(0, r * diagonal, one, 0)

    def exponents(c, scores, top):
        tile = jnp.exp2(scores[c] - top)
        scores[c] = tile
        return folded(tile, jnp.sum)

    def weights(sums, r):
        total = jnp.sum(sums, axis=0, keepdims=True)
        live = lax.broadcasted_iota(jnp.int32, (1, QUERIES), 1) + r * QUERIES < limit
        return jnp.where(live & (total > 0.0), 1.0 / total, 0.0)

    def query_block(r, top, scores, earlier):
        parts = [both_ref[where_ref[r * lanes + i], 0] for i in range(lanes)]
        q_rows = jnp.concatenate(parts, axis=0)

        def product(c):
            k_rows = keys[pl.ds(pl.multiple_of(c * KEYS, KEYS), KEYS), :]
            return (
                lax.dot_general(k_rows, q_rows, (((1,), (1,)), ((), ())), preferred_element_type=jnp.float32)
                * factor
            )

        high = jnp.full((8, QUERIES), -1e30, jnp.float32)
        for d in range(diagonal):
            c = r * diagonal + d
            allowed = (key + d * KEYS <= query) & (key + c * KEYS < limit)
            tile = jnp.where(allowed, product(c), -1e30)
            scores[c] = tile
            high = jnp.maximum(high, folded(tile, jnp.max))

        def step(c, carry):
            high, sums = carry
            tile = product(c)
            scores[c] = tile
            sums = sums + exponents(c, earlier, top)
            return jnp.maximum(high, folded(tile, jnp.max)), sums

        high, sums = lax.fori_loop(0, r * diagonal, step, (high, jnp.zeros((8, QUERIES), jnp.float32)))
        columns(earlier, weights(sums, r - 1), r)
        return jnp.max(high, axis=0, keepdims=True)

    def query_pair(i, top):
        top = query_block(2 * i, top, even, odd)
        return query_block(2 * i + 1, top, odd, even)

    pairs = (limit + 2 * QUERIES - 1) // (2 * QUERIES)
    top = lax.fori_loop(0, pairs, query_pair, jnp.zeros((1, QUERIES), jnp.float32))

    def last_step(c, sums):
        return sums + exponents(c, odd, top)

    sums = lax.fori_loop(0, 2 * pairs * diagonal, last_step, jnp.zeros((8, QUERIES), jnp.float32))
    columns(odd, weights(sums, 2 * pairs - 1), 2 * pairs)

    def store(i, carry):
        p = order_ref[i]
        per = KEYS // BLOCK
        own = col[p // per, pl.ds(pl.multiple_of(lax.rem(p, per) * BLOCK, BLOCK), BLOCK), :]
        out_ref[pl.ds(i, 1), :] = jnp.sum(own.T, axis=0, keepdims=True)
        return carry

    lax.fori_loop(0, blocks, store, 0)


def head_mass(order, limit, both, scale):
    blocks, _, rows, size = both.shape
    tokens = blocks * rows
    smem = pl.BlockSpec(memory_space=pltpu.SMEM)
    vmem = pl.BlockSpec(memory_space=pltpu.VMEM)
    return pl.pallas_call(
        functools.partial(mass_kernel, scale=scale),
        out_shape=jax.ShapeDtypeStruct((blocks, BLOCK), jnp.float32),
        in_specs=[smem, smem, vmem],
        out_specs=vmem,
        scratch_shapes=[
            pltpu.SMEM((blocks,), jnp.int32),
            pltpu.VMEM((tokens, size), jnp.bfloat16),
            pltpu.VMEM((tokens // KEYS, KEYS, QUERIES), jnp.float32),
            pltpu.VMEM((tokens // KEYS, KEYS, QUERIES), jnp.float32),
            pltpu.VMEM((tokens // KEYS, KEYS, BLOCK), jnp.float32),
        ],
        compiler_params=pltpu.CompilerParams(vmem_limit_bytes=48 * 1024 * 1024),
        cost_estimate=pl.CostEstimate(
            flops=2 * tokens * tokens * size, bytes_accessed=4 * tokens * size, transcendentals=tokens * tokens // 2
        ),
        name="head_mass",
    )(order, limit, both)


def by_head_kernel(q_ref, k_ref, out_ref):
    heads, _, _, size = out_ref.shape
    group = q_ref.shape[1] // k_ref.shape[1]
    for h in range(heads):
        g = h // group
        out_ref[h, 0] = q_ref[:, h * size : (h + 1) * size]
        out_ref[h, 1] = k_ref[:, g * size : (g + 1) * size]


def by_head(q_rows, k_rows, size):
    rows, width = q_rows.shape
    vmem = pl.BlockSpec(memory_space=pltpu.VMEM)
    return pl.pallas_call(
        by_head_kernel,
        out_shape=jax.ShapeDtypeStruct((width // size, 2, rows, size), q_rows.dtype),
        in_specs=[vmem, vmem],
        out_specs=vmem,
        compiler_params=pltpu.CompilerParams(vmem_limit_bytes=16 * 1024 * 1024),
        name="by_head",
    )(q_rows, k_rows)


SEQ = ("y", "z", "core")
PLANE = ("y", "z")
SIDE = 4
FINER = 2048.0


def exchanged(array, axis):
    return lax.all_to_all(array, axis, 0, 0, tiled=True)


def shifted(array, axis, by):
    size = lax.axis_size(axis)
    return lax.ppermute(array, axis, [(i, (i + by) % size) for i in range(size)])


def summed(block, axis):
    size = lax.axis_size(axis)
    me = lax.axis_index(axis)
    total = lax.dynamic_index_in_dim(block, me, 0, keepdims=False)
    for by in range(1, size):
        part = lax.dynamic_index_in_dim(block, lax.rem(me + by, size), 0, keepdims=False)
        total = total + shifted(part, axis, by)
    return total


def beside(i):
    return i + 1 - 2 * (i % 2)


def across(i):
    return SIDE - 1 - i


def swapped(array, other):
    return lax.ppermute(array, "batch", [(i, other(i)) for i in range(SIDE)])


def halved(block, first, second):
    me = lax.axis_index("batch")

    def two(i):
        return jnp.stack([lax.dynamic_index_in_dim(block, j, 0, keepdims=False) for j in (i, second(i))])

    return two(me) + swapped(two(first(me)), first)


def finished(kept, second):
    return kept[0] + swapped(kept[1], second)


def in_three(array):
    high = lax.reduce_precision(array, 8, 7)
    middle = lax.reduce_precision(array - high, 8, 7)
    low = array - high - middle
    return jnp.concatenate([high, middle, low], axis=-1).astype(jnp.bfloat16)


def from_three(parts):
    wide = parts.astype(jnp.float32)
    size = wide.shape[-1] // 3
    return wide[..., :size] + wide[..., size : 2 * size] + wide[..., 2 * size :]


def on_device(queries, keys, values, lengths, block_pos, w_in, b_in, output_weight, output_bias):
    q_rows = queries[0]
    k_rows = keys[0]
    v_rows = values[0]
    rows = q_rows.shape[0]
    seq = lax.axis_size(SEQ)
    chips = lax.axis_size(PLANE)
    cores = lax.axis_size("core")
    batch = lax.axis_size("batch")
    heads_kv = output_weight.shape[1]
    hidden = output_weight.shape[0]
    head_size = k_rows.shape[1] // heads_kv
    total = rows * seq
    order = block_pos[0]
    limit = lengths[0]
    chip = lax.axis_index(PLANE)
    core = lax.axis_index("core")

    both = exchanged(by_head(q_rows, k_rows, head_size), SEQ)

    features = jnp.concatenate([q_rows, k_rows, v_rows], axis=1)
    pre = jnp.dot(features, w_in, preferred_element_type=jnp.float32) + b_in
    sig = jax.nn.sigmoid(pre)
    act = (pre * sig).astype(jnp.bfloat16)
    pred = jnp.dot(act, output_weight, preferred_element_type=jnp.float32) + output_bias
    slope = sig * (1.0 + pre * (1.0 - sig))
    largest = jnp.maximum(jnp.max(jnp.abs(slope), axis=1, keepdims=True), 1e-30)
    slope = (slope / largest).astype(jnp.float16)

    width = features.shape[1] // chips
    part = hidden // chips
    carried = jnp.concatenate(
        [
            features.reshape(rows, chips, width),
            act.reshape(rows, chips, part),
            jnp.broadcast_to(
                jnp.pad(
                    jnp.concatenate([in_three(pred), in_three(largest)], axis=1), ((0, 0), (0, part - 3 * heads_kv - 3))
                )[:, None],
                (rows, chips, part),
            ),
        ],
        axis=2,
    )
    both, slope, carried = lax.optimization_barrier((both, slope, jnp.moveaxis(carried, 1, 0)))
    spread = exchanged(carried, PLANE)
    partial = head_mass(order, lengths, both, 1.0 / math.sqrt(head_size))

    by_core = partial.reshape(chips, cores, rows)
    both_heads = lax.dynamic_index_in_dim(by_core, core, 1, keepdims=False)
    both_heads = both_heads + shifted(lax.dynamic_index_in_dim(by_core, 1 - core, 1, keepdims=False), "core", 1)
    high = lax.reduce_precision(both_heads, 5, 10)
    left = (both_heads - high) * FINER
    middle = lax.reduce_precision(left, 5, 10)
    low = (left - middle) * FINER
    carry = jnp.stack([high, middle, low]).astype(jnp.float16).reshape(-1, hidden)
    taken = carry.shape[0]
    carry = jnp.pad(carry, ((0, -taken % 16), (0, 0)))
    arrived = lax.all_gather(jnp.concatenate([slope, carry]), PLANE, axis=0, tiled=False)
    slopes = arrived.reshape(-1, hidden)
    padded = rows + carry.shape[0]
    sums = jnp.sum(
        arrived[:, rows:].astype(jnp.float32).reshape(heads_kv, chips // heads_kv, carry.shape[0], hidden), axis=1
    )
    third = taken // 3
    mass = sums[:, :third] + (sums[:, third : 2 * third] + sums[:, 2 * third : taken] * (1.0 / FINER)) * (1.0 / FINER)
    mass = jnp.pad(mass.reshape(heads_kv, chips, rows), ((0, 0), (0, 0), (0, padded - rows)))
    labels = jnp.log1p(mass.reshape(heads_kv, chips * padded)).T

    spread = jnp.pad(spread, ((0, 0), (0, padded - rows), (0, 0))).reshape(chips * padded, width + 2 * part)
    feats = spread[:, :width]
    acts = spread[:, width : width + part]
    predicted = from_three(spread[:, width + part : width + part + 3 * heads_kv])
    factor = from_three(spread[:, width + part + 3 * heads_kv : width + part + 3 * heads_kv + 3])
    offsets = jnp.arange(rows, dtype=jnp.int32)
    blocks = lax.dynamic_index_in_dim(order.reshape(chips, cores), core, 1, keepdims=False)
    position = (blocks[:, None] * rows + offsets[None, :]).reshape(-1)
    live = (position < limit).astype(jnp.float32)
    live = jnp.pad(live.reshape(chips, rows), ((0, 0), (0, padded - rows))).reshape(-1)
    norm = 1.0 / math.sqrt(batch * total)
    resid = ((predicted - labels) * live[:, None] * norm).astype(jnp.bfloat16)
    back = lax.dot_general(
        resid, output_weight, (((1,), (1,)), ((), ())), preferred_element_type=jnp.float32
    )
    delta = (back * (slopes.astype(jnp.float32) * factor)).astype(jnp.bfloat16)
    out_part = lax.dot_general(acts, resid, (((0,), (0,)), ((), ())), preferred_element_type=jnp.float32)
    b_part = lax.dynamic_index_in_dim(
        jnp.sum(delta.astype(jnp.float32), axis=0).reshape(chips, part), chip, 0, keepdims=False
    )
    small = jnp.concatenate([out_part.ravel(), b_part, jnp.sum(resid.astype(jnp.float32), axis=0)])
    size = small.shape[0]
    small = jnp.pad(small, (0, -size % 128))
    small = exchanged(jnp.broadcast_to(small[None], (seq, small.shape[0])), SEQ)
    block = lax.dot_general(
        feats, delta, (((0,), (0,)), ((), ())), preferred_element_type=jnp.float32
    )
    block = summed(block.reshape(cores, width // cores, hidden), "core")
    block = block.reshape(batch, width // (cores * batch), hidden)
    half = hidden // 2
    kept = [halved(block[:, :, :half], beside, across), halved(block[:, :, half:], across, beside)]
    grad_w_in = jnp.concatenate([finished(kept[0], across), finished(kept[1], beside)], axis=1)
    small = jnp.sum(small.reshape(chips, cores, small.shape[1]), axis=1)
    small = small + sum(shifted(small, "batch", by) for by in range(1, batch))
    output_weight_gradient = small[:, : part * heads_kv].reshape(hidden, heads_kv)
    grad_b_in = small[:, part * heads_kv : part * heads_kv + part].reshape(hidden)
    output_bias_gradient = small[0, part * heads_kv + part : size]
    return (grad_w_in, grad_b_in, output_weight_gradient, output_bias_gradient)


def solution(mesh):
    cores = mesh.shape["seq"] // (SIDE * SIDE)
    fine = Mesh(
        mesh.devices.reshape(SIDE, SIDE, cores, mesh.shape["batch"]), SEQ + ("batch",)
    )
    return jax.shard_map(
        on_device,
        mesh=fine,
        in_specs=(
            P("batch", SEQ, None),
            P("batch", SEQ, None),
            P("batch", SEQ, None),
            P("batch"),
            P("batch", None),
            P(),
            P(),
            P(),
            P(),
        ),
        out_specs=(P(SEQ + ("batch",), None), P(), P(), P()),
        check_vma=False,
    )
```

```python
import functools
import math

import jax
import jax.numpy as jnp
from jax import lax
from jax.experimental import pallas as pl
from jax.experimental.pallas import tpu as pltpu
from jax.sharding import Mesh
from jax.sharding import PartitionSpec as P

BLOCK = 128
QUERIES = 512
KEYS = 512


def mass_kernel(order_ref, limit_ref, core_ref, both_ref, other_ref, out_ref, where_ref, keys, even, odd, col, *, scale):
    blocks = both_ref.shape[0]
    limit = limit_ref[0]
    factor = scale * math.log2(math.e)
    diagonal = QUERIES // KEYS
    lanes = QUERIES // BLOCK

    def by_position(i, carry):
        p = order_ref[i]
        where_ref[p] = i
        part = other_ref.shape[1]
        mine = pl.multiple_of(p * BLOCK + core_ref[0] * part, part)
        theirs = pl.multiple_of(p * BLOCK + (1 - core_ref[0]) * part, part)
        keys[pl.ds(mine, part), :] = both_ref[i, BLOCK:]
        keys[pl.ds(theirs, part), :] = other_ref[i]
        return carry

    lax.fori_loop(0, blocks, by_position, 0)
    col[...] = jnp.zeros_like(col)
    key = lax.broadcasted_iota(jnp.int32, (KEYS, QUERIES), 0)
    query = lax.broadcasted_iota(jnp.int32, (KEYS, QUERIES), 1)

    def folded(tile, op):
        return op(tile.reshape(KEYS // 8, 8, QUERIES), axis=0)

    def column_step(c, scores, weight):
        tile = scores[c] * weight
        part = tile[:, :BLOCK]
        for i in range(1, lanes):
            part = part + tile[:, i * BLOCK : (i + 1) * BLOCK]
        col[c] += part

    def columns(scores, weight, r):
        def one(c, carry):
            column_step(c, scores, weight)
            return carry

        lax.fori_loop(0, r * diagonal, one, 0)

    def exponents(c, scores, top):
        tile = jnp.exp2(scores[c] - top)
        scores[c] = tile
        return folded(tile, jnp.sum)

    def weights(sums, r):
        total = jnp.sum(sums, axis=0, keepdims=True)
        live = lax.broadcasted_iota(jnp.int32, (1, QUERIES), 1) + r * QUERIES < limit
        return jnp.where(live & (total > 0.0), 1.0 / total, 0.0)

    def query_block(r, top, scores, earlier):
        parts = [both_ref[where_ref[r * lanes + i], :BLOCK] for i in range(lanes)]
        q_rows = jnp.concatenate(parts, axis=0)

        def product(c):
            k_rows = keys[pl.ds(pl.multiple_of(c * KEYS, KEYS), KEYS), :]
            return (
                lax.dot_general(k_rows, q_rows, (((1,), (1,)), ((), ())), preferred_element_type=jnp.float32)
                * factor
            )

        high = jnp.full((8, QUERIES), -1e30, jnp.float32)
        for d in range(diagonal):
            c = r * diagonal + d
            allowed = (key + d * KEYS <= query) & (key + c * KEYS < limit)
            tile = jnp.where(allowed, product(c), -1e30)
            scores[c] = tile
            high = jnp.maximum(high, folded(tile, jnp.max))

        def step(c, carry):
            high, sums = carry
            tile = product(c)
            scores[c] = tile
            sums = sums + exponents(c, earlier, top)
            return jnp.maximum(high, folded(tile, jnp.max)), sums

        high, sums = lax.fori_loop(0, r * diagonal, step, (high, jnp.zeros((8, QUERIES), jnp.float32)))
        columns(earlier, weights(sums, r - 1), r)
        return jnp.max(high, axis=0, keepdims=True)

    def query_pair(i, top):
        top = query_block(2 * i, top, even, odd)
        return query_block(2 * i + 1, top, odd, even)

    pairs = (limit + 2 * QUERIES - 1) // (2 * QUERIES)
    top = lax.fori_loop(0, pairs, query_pair, jnp.zeros((1, QUERIES), jnp.float32))

    def last_step(c, sums):
        return sums + exponents(c, odd, top)

    sums = lax.fori_loop(0, 2 * pairs * diagonal, last_step, jnp.zeros((8, QUERIES), jnp.float32))
    columns(odd, weights(sums, 2 * pairs - 1), 2 * pairs)

    def store(i, carry):
        p = order_ref[i]
        per = KEYS // BLOCK
        own = col[p // per, pl.ds(pl.multiple_of(lax.rem(p, per) * BLOCK, BLOCK), BLOCK), :]
        out_ref[pl.ds(i, 1), :] = jnp.sum(own.T, axis=0, keepdims=True)
        return carry

    lax.fori_loop(0, blocks, store, 0)


def head_mass(order, limit, core, both, other, scale):
    blocks, _, size = both.shape
    tokens = blocks * BLOCK
    smem = pl.BlockSpec(memory_space=pltpu.SMEM)
    vmem = pl.BlockSpec(memory_space=pltpu.VMEM)
    return pl.pallas_call(
        functools.partial(mass_kernel, scale=scale),
        out_shape=jax.ShapeDtypeStruct((blocks, BLOCK), jnp.float32),
        in_specs=[smem, smem, smem, vmem, vmem],
        out_specs=vmem,
        scratch_shapes=[
            pltpu.SMEM((blocks,), jnp.int32),
            pltpu.VMEM((tokens, size), jnp.bfloat16),
            pltpu.VMEM((tokens // KEYS, KEYS, QUERIES), jnp.float32),
            pltpu.VMEM((tokens // KEYS, KEYS, QUERIES), jnp.float32),
            pltpu.VMEM((tokens // KEYS, KEYS, BLOCK), jnp.float32),
        ],
        compiler_params=pltpu.CompilerParams(vmem_limit_bytes=48 * 1024 * 1024),
        cost_estimate=pl.CostEstimate(
            flops=2 * tokens * tokens * size, bytes_accessed=4 * tokens * size, transcendentals=tokens * tokens // 2
        ),
        name="head_mass",
    )(order, limit, core, both, other)


def by_head_kernel(q_ref, k_ref, out_ref):
    heads, _, size = out_ref.shape
    rows = q_ref.shape[0]
    group = q_ref.shape[1] // k_ref.shape[1]
    for h in range(heads):
        g, c = h // group, h % 2
        out_ref[h, :rows] = q_ref[:, h * size : (h + 1) * size]
        out_ref[h, rows:] = k_ref[c * rows // 2 : (c + 1) * rows // 2, g * size : (g + 1) * size]


def by_head(q_rows, k_rows, size):
    rows, width = q_rows.shape
    vmem = pl.BlockSpec(memory_space=pltpu.VMEM)
    return pl.pallas_call(
        by_head_kernel,
        out_shape=jax.ShapeDtypeStruct((width // size, rows + rows // 2, size), q_rows.dtype),
        in_specs=[vmem, vmem],
        out_specs=vmem,
        compiler_params=pltpu.CompilerParams(vmem_limit_bytes=16 * 1024 * 1024),
        name="by_head",
    )(q_rows, k_rows)


SEQ = ("y", "z", "core")
PLANE = ("y", "z")
SIDE = 4
FINER = 2048.0


def exchanged(array, axis):
    return lax.all_to_all(array, axis, 0, 0, tiled=True)


def shifted(array, axis, by):
    size = lax.axis_size(axis)
    return lax.ppermute(array, axis, [(i, (i + by) % size) for i in range(size)])


def summed(block, axis):
    size = lax.axis_size(axis)
    me = lax.axis_index(axis)
    total = lax.dynamic_index_in_dim(block, me, 0, keepdims=False)
    for by in range(1, size):
        part = lax.dynamic_index_in_dim(block, lax.rem(me + by, size), 0, keepdims=False)
        total = total + shifted(part, axis, by)
    return total


def beside(i):
    return i + 1 - 2 * (i % 2)


def across(i):
    return SIDE - 1 - i


def swapped(array, other):
    return lax.ppermute(array, "batch", [(i, other(i)) for i in range(SIDE)])


def halved(block, first, second):
    me = lax.axis_index("batch")

    def two(i):
        return jnp.stack([lax.dynamic_index_in_dim(block, j, 0, keepdims=False) for j in (i, second(i))])

    return two(me) + swapped(two(first(me)), first)


def finished(kept, second):
    return kept[0] + swapped(kept[1], second)


def in_three(array):
    high = lax.reduce_precision(array, 8, 7)
    middle = lax.reduce_precision(array - high, 8, 7)
    low = array - high - middle
    return jnp.concatenate([high, middle, low], axis=-1).astype(jnp.bfloat16)


def from_three(parts):
    wide = parts.astype(jnp.float32)
    size = wide.shape[-1] // 3
    return wide[..., :size] + wide[..., size : 2 * size] + wide[..., 2 * size :]


def on_device(queries, keys, values, lengths, block_pos, w_in, b_in, output_weight, output_bias):
    q_rows = queries[0]
    k_rows = keys[0]
    v_rows = values[0]
    rows = q_rows.shape[0]
    seq = lax.axis_size(SEQ)
    chips = lax.axis_size(PLANE)
    cores = lax.axis_size("core")
    batch = lax.axis_size("batch")
    heads_kv = output_weight.shape[1]
    hidden = output_weight.shape[0]
    head_size = k_rows.shape[1] // heads_kv
    total = rows * seq
    order = block_pos[0]
    limit = lengths[0]
    chip = lax.axis_index(PLANE)
    core = lax.axis_index("core")

    both = exchanged(by_head(q_rows, k_rows, head_size), SEQ)

    features = jnp.concatenate([q_rows, k_rows, v_rows], axis=1)
    pre = jnp.dot(features, w_in, preferred_element_type=jnp.float32) + b_in
    sig = jax.nn.sigmoid(pre)
    act = (pre * sig).astype(jnp.bfloat16)
    pred = jnp.dot(act, output_weight, preferred_element_type=jnp.float32) + output_bias
    slope = sig * (1.0 + pre * (1.0 - sig))
    largest = jnp.maximum(jnp.max(jnp.abs(slope), axis=1, keepdims=True), 1e-30)
    slope = (slope / largest).astype(jnp.float16)

    width = features.shape[1] // chips
    part = hidden // chips
    carried = jnp.concatenate(
        [
            features.reshape(rows, chips, width),
            act.reshape(rows, chips, part),
            jnp.broadcast_to(
                jnp.pad(
                    jnp.concatenate([in_three(pred), in_three(largest)], axis=1), ((0, 0), (0, part - 3 * heads_kv - 3))
                )[:, None],
                (rows, chips, part),
            ),
        ],
        axis=2,
    )
    other = shifted(both[:, rows:], "core", 1)
    both, other, slope, carried = lax.optimization_barrier((both, other, slope, jnp.moveaxis(carried, 1, 0)))
    spread = exchanged(carried, PLANE)
    partial = head_mass(order, lengths, core.reshape(1).astype(jnp.int32), both, other, 1.0 / math.sqrt(head_size))

    by_core = partial.reshape(chips, cores, rows)
    both_heads = lax.dynamic_index_in_dim(by_core, core, 1, keepdims=False)
    both_heads = both_heads + shifted(lax.dynamic_index_in_dim(by_core, 1 - core, 1, keepdims=False), "core", 1)
    high = lax.reduce_precision(both_heads, 5, 10)
    left = (both_heads - high) * FINER
    middle = lax.reduce_precision(left, 5, 10)
    low = (left - middle) * FINER
    carry = jnp.stack([high, middle, low]).astype(jnp.float16).reshape(-1, hidden)
    taken = carry.shape[0]
    carry = jnp.pad(carry, ((0, -taken % 16), (0, 0)))
    arrived = lax.all_gather(jnp.concatenate([slope, carry]), PLANE, axis=0, tiled=False)
    slopes = arrived.reshape(-1, hidden)
    padded = rows + carry.shape[0]
    sums = jnp.sum(
        arrived[:, rows:].astype(jnp.float32).reshape(heads_kv, chips // heads_kv, carry.shape[0], hidden), axis=1
    )
    third = taken // 3
    mass = sums[:, :third] + (sums[:, third : 2 * third] + sums[:, 2 * third : taken] * (1.0 / FINER)) * (1.0 / FINER)
    mass = jnp.pad(mass.reshape(heads_kv, chips, rows), ((0, 0), (0, 0), (0, padded - rows)))
    labels = jnp.log1p(mass.reshape(heads_kv, chips * padded)).T

    spread = jnp.pad(spread, ((0, 0), (0, padded - rows), (0, 0))).reshape(chips * padded, width + 2 * part)
    feats = spread[:, :width]
    acts = spread[:, width : width + part]
    predicted = from_three(spread[:, width + part : width + part + 3 * heads_kv])
    factor = from_three(spread[:, width + part + 3 * heads_kv : width + part + 3 * heads_kv + 3])
    offsets = jnp.arange(rows, dtype=jnp.int32)
    blocks = lax.dynamic_index_in_dim(order.reshape(chips, cores), core, 1, keepdims=False)
    position = (blocks[:, None] * rows + offsets[None, :]).reshape(-1)
    live = (position < limit).astype(jnp.float32)
    live = jnp.pad(live.reshape(chips, rows), ((0, 0), (0, padded - rows))).reshape(-1)
    norm = 1.0 / math.sqrt(batch * total)
    resid = ((predicted - labels) * live[:, None] * norm).astype(jnp.bfloat16)
    back = lax.dot_general(
        resid, output_weight, (((1,), (1,)), ((), ())), preferred_element_type=jnp.float32
    )
    delta = (back * (slopes.astype(jnp.float32) * factor)).astype(jnp.bfloat16)
    out_part = lax.dot_general(acts, resid, (((0,), (0,)), ((), ())), preferred_element_type=jnp.float32)
    b_part = lax.dynamic_index_in_dim(
        jnp.sum(delta.astype(jnp.float32), axis=0).reshape(chips, part), chip, 0, keepdims=False
    )
    small = jnp.concatenate([out_part.ravel(), b_part, jnp.sum(resid.astype(jnp.float32), axis=0)])
    size = small.shape[0]
    small = jnp.pad(small, (0, -size % 128))
    small = exchanged(jnp.broadcast_to(small[None], (seq, small.shape[0])), SEQ)
    block = lax.dot_general(
        feats, delta, (((0,), (0,)), ((), ())), preferred_element_type=jnp.float32
    )
    block = summed(block.reshape(cores, width // cores, hidden), "core")
    block = block.reshape(batch, width // (cores * batch), hidden)
    half = hidden // 2
    kept = [halved(block[:, :, :half], beside, across), halved(block[:, :, half:], across, beside)]
    grad_w_in = jnp.concatenate([finished(kept[0], across), finished(kept[1], beside)], axis=1)
    small = jnp.sum(small.reshape(chips, cores, small.shape[1]), axis=1)
    small = small + sum(shifted(small, "batch", by) for by in range(1, batch))
    output_weight_gradient = small[:, : part * heads_kv].reshape(hidden, heads_kv)
    grad_b_in = small[:, part * heads_kv : part * heads_kv + part].reshape(hidden)
    output_bias_gradient = small[0, part * heads_kv + part : size]
    return (grad_w_in, grad_b_in, output_weight_gradient, output_bias_gradient)


def solution(mesh):
    cores = mesh.shape["seq"] // (SIDE * SIDE)
    fine = Mesh(
        mesh.devices.reshape(SIDE, SIDE, cores, mesh.shape["batch"]), SEQ + ("batch",)
    )
    return jax.shard_map(
        on_device,
        mesh=fine,
        in_specs=(
            P("batch", SEQ, None),
            P("batch", SEQ, None),
            P("batch", SEQ, None),
            P("batch"),
            P("batch", None),
            P(),
            P(),
            P(),
            P(),
        ),
        out_specs=(P(SEQ + ("batch",), None), P(), P(), P()),
        check_vma=False,
    )
```
